32 devices in a mesh: gx: 4 (over y, x), gy: 4 (over z), gz: 2 (over core).
Axes of the slice: x: 2, y: 2, z: 4, core: 2. Of those that a mesh axis runs over, the one named last changes fastest.
Arguments:
- fields: bfloat16 [4096, 2048], P(('gx', 'gy', 'gz')), may hold values from -6 to 6
- coordinates: float32 [3, 524288], P(None, ('gx', 'gy', 'gz')), may hold values from -1 to 1
- element_rank: int32 [524288, 1], P(('gx', 'gy', 'gz')), may hold values from 0 to 31; in each aligned block of 16384 rows (0 to 16383, 16384 to 32767, ...) at most 640 rows name the same one
- element_slot: int32 [524288], P(('gx', 'gy', 'gz')), may hold values from 0 to 127
Outputs:
- samples: float32 [4, 524288], P(None, ('gx', 'gy', 'gz'))
The draws below stay inside these ranges and needn't reach their ends.
Inputs may be any that keep to these rules, and one draw needn't show every extreme that they name: `element_rank`: among the probes of one device no rank is named by more than 640 probes, and in some devices' blocks one rank is named by exactly 640.
All inputs are finite; a program needn't handle non-finite values.
Results may differ from the reference program's by a relative error of at most 0.0024.
Values sent between devices are 32-bit elements; how exact they have to be, the bound alone decides.
No kernel may reach another device: no remote copies, remote signals or barrier semaphores. Data moves between devices by JAX's collectives and lax.ppermute only.
A program may use at most 64 MiB of HBM per device.

```python
import math
import jax
import jax.numpy as jnp
import numpy as np
from jax import lax

ROW = 2048
E_DEV = 128
P_DEV = 16384
CAP = 640
ELEMENTS = 4096
PROBES = 524288
DEVICES = 32


def place_ends(values, key, least, largest):
    longest = values.shape.index(max(values.shape))
    spots = []
    for shift in (0, 1):
        where = [jax.random.randint(jax.random.fold_in(key, axis), (), 0, length) for axis, length in enumerate(values.shape)]
        where[longest] = (where[longest] + shift) % values.shape[longest]
        spots.append(tuple(where))
    return values.at[spots[0]].set(least).at[spots[1]].set(largest)


def shard_levels(rng, dims, split, least, largest):
    loudness = 1.0
    for axis_at, parts in split:
        heights = jax.random.uniform(jax.random.fold_in(jax.random.fold_in(rng, 6), axis_at), (parts,), jnp.float32, least / len(split), largest / len(split))
        loudness = loudness * jnp.repeat(jnp.exp(heights), dims[axis_at] // parts).reshape((-1,) + (1,) * (len(dims) - 1 - axis_at))
    return loudness


def routed_block(key, own, number, rows, count, top, most, slope):
    sequence = jax.random.permutation(key, count)
    packed, usual = shares(count, rows * top, most, slope, True), shares(count, rows * top, most, slope, False)
    places = jnp.arange(count)

    def named(sizes, turn):
        used = int((sizes > 0).sum())
        fixed = max(1, used // 4)
        shifted = fixed + (places - fixed + turn * (used - fixed)) % max(1, count - fixed)
        return jnp.zeros((count,), jnp.int32).at[sequence[jnp.where(places < fixed, places, shifted)]].set(jnp.asarray(sizes, jnp.int32))

    sizes = jnp.where(number % 4 == 0, named(packed, number // 4), named(usual, number - number // 4 - 1))
    mixed = jax.random.permutation(jax.random.fold_in(own, 3), count)
    source_of, sink = mixed[0:count // 2 * 2:2], mixed[1:count // 2 * 2:2]
    margin = jnp.minimum(sizes[source_of] - 1, most - sizes[sink]) // 2
    margin = jnp.where((source_of == sequence[0]) | (sink == sequence[0]) | (sizes[sink] == 0), 0, jnp.maximum(margin, 0))
    shifted = jax.random.randint(jax.random.fold_in(own, 4), (count // 2,), 0, 1 << 20) % (margin + 1)
    sizes = sizes.at[source_of].add(-shifted).at[sink].add(shifted)
    labels = jnp.searchsorted(jnp.cumsum(sizes), jnp.arange(rows * top), side="right").astype(jnp.int32)
    listing = labels.reshape(top, rows).T
    listing = listing[jax.random.permutation(jax.random.fold_in(own, 1), rows)]
    turn = jax.random.randint(jax.random.fold_in(own, 2), (rows, 1), 0, top)
    return jnp.take_along_axis(listing, (jnp.arange(top)[None, :] + turn) % top, axis=1)


def shares(count, total, bound, skew, full):
    loads = [(1 << 20) // math.isqrt(standing ** skew) + 1 for standing in range(1, count + 1)]
    largest = bound if full else min(bound, max(-(-total // count), total * loads[0] // sum(loads)))
    least = 1 if total - largest >= count - 1 else 0
    given, rest = [largest] + [least] * (count - 1), total - largest - least * (count - 1)
    while rest > 0:
        free = [i for i in range(1, count) if given[i] < largest] or [i for i in range(1, count) if given[i] < bound]
        pool, remaining = sum([loads[i] for i in free]), rest
        for i in free:
            addition = min(bound - given[i], max(1, remaining * loads[i] // pool), rest)
            given[i] = given[i] + addition
            rest = rest - addition
    return np.array(given)


def bell_draw(own_key, extent, spread, most, shards=(), held_as=jnp.bfloat16):
    drawn = jax.random.normal(own_key, extent, jnp.float32) * spread
    if len(shards) > 0:
        drawn = shard_levels(own_key, extent, shards, -0.22, 0.18) * drawn
    return jnp.clip(drawn, min=-most, max=most).astype(held_as)


def setup_inputs(seed: int = 0) -> dict:
    arg_keys = jax.random.split(jax.random.key(seed), 5)
    fields = bell_draw(arg_keys[0], (ELEMENTS, ROW), 1.0, 6.0, ((0, 32),))
    coordinates = jnp.clip(jax.random.uniform(arg_keys[1], (3, PROBES), jnp.float32, -1.0, 1.0) * shard_levels(arg_keys[1], (3, PROBES), ((1, 32),), -0.4, 0.0), -1.0, 1.0)
    element_rank_keys = jax.random.split(jax.random.fold_in(arg_keys[2], 1), PROBES // P_DEV)
    element_rank_turns = jax.random.permutation(jax.random.fold_in(arg_keys[2], 3), PROBES // P_DEV)
    element_rank = jax.vmap(lambda own, number: routed_block(jax.random.fold_in(arg_keys[2], 2), own, number, P_DEV, DEVICES, 1, CAP, 2))(element_rank_keys, element_rank_turns).reshape((PROBES, 1))
    element_slot = place_ends(jax.random.randint(arg_keys[3], (PROBES,), 0, E_DEV), jax.random.fold_in(arg_keys[3], 1), 0, E_DEV - 1).astype(jnp.int32)
    return {"fields": fields, "coordinates": coordinates, "element_rank": element_rank, "element_slot": element_slot}


gll_points = np.array([-1.0, -0.8717401485096066, -0.5917001814331423, -0.2092992179024789, 0.2092992179024789, 0.5917001814331423, 0.8717401485096066, 1.0])
gll_scale = np.array([1.0 / np.prod([gll_points[a] - gll_points[b] for b in range(8) if b != a]) for a in range(8)])


def lagrange(coord):
    offsets = coord[None, :] - jnp.asarray(gll_points, coord.dtype)[:, None]
    weights = []
    for node_a in range(8):
        factor = jnp.ones_like(coord) * gll_scale[node_a]
        for node_b in range(8):
            if node_b != node_a:
                factor = factor * offsets[node_b]
        weights.append(factor)
    return jnp.stack(weights, axis=0)


def interpolate(coordinates, element, fields):
    total_rows = element.shape[0]
    block_rows = math.gcd(total_rows, 8192)
    block_count = total_rows // block_rows

    def one_block(pieces):
        coords_block, slots_block = pieces
        weight_r = lagrange(coords_block[0])
        weight_s = lagrange(coords_block[1])
        weight_t = lagrange(coords_block[2]).astype(jnp.bfloat16)
        gathered = jnp.take(fields, slots_block, axis=0).reshape(block_rows, 256, 8)
        along_t = jnp.einsum("nak,kn->na", gathered.astype(jnp.float32), weight_t.astype(jnp.float32), precision=lax.Precision.HIGHEST)
        along_t = along_t.reshape(block_rows, 4, 8, 8)
        along_s = jnp.einsum("nfij,jn->nfi", along_t, weight_s, precision=lax.Precision.HIGHEST)
        return jnp.einsum("nfi,in->fn", along_s, weight_r, precision=lax.Precision.HIGHEST)

    coords_blocks = coordinates.reshape(3, block_count, block_rows).transpose(1, 0, 2)
    slot_blocks = element.reshape(block_count, block_rows)
    result = lax.map(one_block, (coords_blocks, slot_blocks))
    return result.transpose(1, 0, 2).reshape(4, total_rows)


def reference(fields, coordinates, element_rank, element_slot):
    element = element_rank[:, 0].astype(jnp.int32) * E_DEV + element_slot.astype(jnp.int32)
    return interpolate(coordinates, element, fields)
```

```python
import functools
import math

import jax
import jax.numpy as jnp
import numpy as np
from jax import lax
from jax.experimental import pallas as pl
from jax.experimental.pallas import tpu as pltpu
from jax.sharding import PartitionSpec as P

LANES = 128

gll_points = np.array([-1.0,-0.8717401485096066,-0.5917001814331423,-0.2092992179024789,0.2092992179024789,0.5917001814331423,0.8717401485096066,1.0])
gll_scale = np.array([1.0 / np.prod([gll_points[a] - gll_points[b] for b in range(8) if b != a]) for a in range(8)])

def lagrange_rows(coord, scale, node):
    weights = jnp.broadcast_to(scale, node.shape)
    for b in range(8):
        offset = coord - np.float32(gll_points[b])
        weights = weights * jnp.where(node == b, np.float32(1.0), offset)
    return weights

def evaluate_kernel(table_ref, probes_ref, samples_ref, *, step):
    groups, _, width = probes_ref.shape
    elements = table_ref.shape[1] // 8
    rows = jnp.concatenate([probes_ref[g] for g in range(groups)], axis=1)
    node = lax.broadcasted_iota(jnp.int32, (8, step), 0)
    scale = jnp.full((8, step), gll_scale[0], jnp.float32)
    for a in range(1, 8):
        scale = jnp.where(node == a, np.float32(gll_scale[a]), scale)
    ids = lax.broadcasted_iota(jnp.int32, (elements, step), 0).astype(jnp.float32).astype(jnp.bfloat16)
    total = groups * width
    parts = []
    for at in range(0, total, step):
        block = rows[:, at:at + step]
        weight_r = lagrange_rows(block[0:1], scale, node)
        weight_s = lagrange_rows(block[1:2], scale, node)
        weight_t = lagrange_rows(block[2:3], scale, node)
        slot = jnp.broadcast_to(block[3:4], (elements, step)).astype(jnp.bfloat16)
        mine = slot == ids
        right = []
        for c in range(8):
            w = jnp.broadcast_to(weight_t[c:c + 1], (elements, step)).astype(jnp.bfloat16)
            right.append(jnp.where(mine, w, jnp.zeros_like(w)))
        right = jnp.concatenate(right, axis=0)
        along_t = jnp.dot(table_ref[...], right, preferred_element_type=jnp.float32)
        out = []
        for f in range(4):
            acc = None
            for b in range(8):
                at_b = (f * 8 + b) * 8
                term = along_t[at_b:at_b + 8] * weight_s[b:b + 1]
                acc = term if acc is None else acc + term
            out.append(jnp.sum(acc * weight_r, axis=0, keepdims=True))
        parts.append(jnp.concatenate(out, axis=0))
    full = jnp.concatenate(parts, axis=1)
    for g in range(groups):
        samples_ref[g] = full[:, g * width:(g + 1) * width]

def evaluate(probes, fields, groups=4, step=256):
    devices, _, width = probes.shape
    elements = fields.shape[0]
    table = fields.reshape(elements, 4, 8, 8, 8).transpose(1, 3, 2, 4, 0).reshape(256, 8 * elements)
    spec = pl.BlockSpec((groups, 4, width), lambda i: (i, 0, 0))
    n = devices * width
    return pl.pallas_call(
        functools.partial(evaluate_kernel, step=step),
        grid=(devices // groups,),
        in_specs=[pl.BlockSpec((256, 8 * elements), lambda i: (0, 0)), spec],
        out_specs=spec,
        out_shape=jax.ShapeDtypeStruct(probes.shape, jnp.float32),
        cost_estimate=pl.CostEstimate(flops=2 * n * 256 * 8 * elements, bytes_accessed=8 * n * 4, transcendentals=0),
        name="evaluate",
    )(table, probes)

def split_rows(x):
    high = x.astype(jnp.bfloat16)
    rest = x - high.astype(jnp.float32)
    middle = rest.astype(jnp.bfloat16)
    low = (rest - middle.astype(jnp.float32)).astype(jnp.bfloat16)
    return jnp.concatenate([high, middle, low, jnp.zeros_like(low)], axis=0)

def join_rows(y):
    return y[0:8] + y[8:16] + y[16:24]

def count_kernel(target_ref, place_ref, starts_ref, picks_ref, sums_ref, *, ranks, window):
    blocks, _, rows = target_ref.shape
    ident = lax.broadcasted_iota(jnp.int32, (ranks, rows), 0)
    for k in range(blocks):
        mine = jnp.broadcast_to(target_ref[k], (ranks, rows)) == ident
        picks_ref[k * ranks:(k + 1) * ranks, :] = jnp.where(mine, 1.0, 0.0).astype(jnp.bfloat16)
    upper = lax.broadcasted_iota(jnp.int32, (rows, rows), 0) <= lax.broadcasted_iota(jnp.int32, (rows, rows), 1)
    upper = jnp.where(upper, 1.0, 0.0).astype(jnp.bfloat16)
    sums_ref[...] = jnp.dot(picks_ref[...], upper, preferred_element_type=jnp.float32)
    lane = lax.broadcasted_iota(jnp.int32, (ranks, LANES), 1)
    running = jnp.zeros((ranks, 1), jnp.float32)
    table = jnp.zeros((ranks, LANES), jnp.float32)
    most = jnp.zeros((1, LANES), jnp.float32)
    for k in range(blocks):
        at = slice(k * ranks, (k + 1) * ranks)
        target = target_ref[k]
        mine = jnp.broadcast_to(target, (ranks, rows)) == ident
        within = jnp.sum(jnp.where(mine, sums_ref[at, :], 0.0), axis=0, keepdims=True) - 1.0
        place_ref[k] = (target * (1 << 16)) + within.astype(jnp.int32)
        counts = sums_ref[at, rows - 1:rows]
        table = jnp.where(lane == k, running, table)
        most = jnp.where(lane[0:1] == k, jnp.max(counts, axis=0, keepdims=True), most)
        running = running + counts
    table = jnp.where(lane == blocks, running, table)
    starts_ref[0:ranks, :] = table.astype(jnp.int32)
    starts_ref[ranks:ranks + 1, :] = most.astype(jnp.int32)

def count(target, ranks, window):
    blocks, _, rows = target.shape
    return pl.pallas_call(
        functools.partial(count_kernel, ranks=ranks, window=window),
        out_shape=(jax.ShapeDtypeStruct((blocks, 1, rows), jnp.int32), jax.ShapeDtypeStruct((ranks + 8, LANES), jnp.int32)),
        scratch_shapes=[pltpu.VMEM((blocks * ranks, rows), jnp.bfloat16), pltpu.VMEM((blocks * ranks, rows), jnp.float32)],
        name="count",
    )(target)

def one_hot(place, ranks, window, turn):
    rank = lax.shift_right_logical(place, 16)
    order = (place & 0xFFFF) - turn * window
    index = jnp.where((order >= 0) & (order < window), rank * window + order, -1)
    rows = place.shape[1]
    index = jnp.broadcast_to(index, (16, rows)).astype(jnp.int16)
    base = lax.broadcasted_iota(jnp.int32, (16, rows), 0).astype(jnp.int16)
    out = []
    for p in range(0, ranks * window, 16):
        out.append(jnp.where(index == base + np.int16(p), jnp.ones((16, rows), jnp.bfloat16), jnp.zeros((16, rows), jnp.bfloat16)))
    return jnp.concatenate(out, axis=0)

def pack_kernel(starts_ref, coordinates_ref, slot_ref, place_ref, out_ref, buffer_ref, *, ranks, window, tiles, unroll):
    blocks, _, rows = place_ref.shape
    stride = tiles + 2
    per_tile = LANES // window
    lane = lax.broadcasted_iota(jnp.int32, (8, LANES), 1)

    def clear(i, _):
        buffer_ref[i] = jnp.zeros((8, LANES), jnp.float32)
        return 0
    lax.fori_loop(0, ranks * stride, clear, 0, unroll=8)

    def payload(k):
        at = pl.ds(pl.multiple_of(k * rows, LANES), rows)
        return jnp.concatenate([coordinates_ref[:, at], slot_ref[k].astype(jnp.float32), jnp.zeros((4, rows), jnp.float32)], axis=0)

    def sort(k, turn):
        hot = one_hot(place_ref[k], ranks, window, turn)
        left = split_rows(payload(k))
        return join_rows(lax.dot_general(left, hot, (((1,), (1,)), ((), ())), preferred_element_type=jnp.float32))

    def main(g, _):
        for u in range(unroll):
            k = g * unroll + u
            ordered = sort(k, 0)
            for d in range(ranks):
                q, at = d // per_tile, (d % per_tile) * window
                start = starts_ref[d, k]
                tile, low = lax.shift_right_logical(start, 7), start & (LANES - 1)
                moved = pltpu.roll(ordered[:, q * LANES:(q + 1) * LANES], (low - at) & (LANES - 1), 1)
                cell = d * stride + tile
                buffer_ref[cell] = jnp.where(lane < low, buffer_ref[cell], moved)
                buffer_ref[cell + 1] = moved
        return 0
    lax.fori_loop(0, blocks // unroll, main, 0)

    def repair(k, _):
        def turn_body(turn, _):
            ordered = sort(k, turn)
            for d in range(ranks):
                q, at = d // per_tile, (d % per_tile) * window
                start = starts_ref[d, k]
                length = starts_ref[d, k + 1] - start
                first = jnp.minimum(turn * window, length)
                size = jnp.minimum(length - first, window)
                start = start + first
                tile, low = lax.shift_right_logical(start, 7), start & (LANES - 1)
                moved = pltpu.roll(ordered[:, q * LANES:(q + 1) * LANES], (low - at) & (LANES - 1), 1)
                cell = d * stride + tile
                buffer_ref[cell] = jnp.where((lane >= low) & (lane < low + size), moved, buffer_ref[cell])
                buffer_ref[cell + 1] = jnp.where(lane < low + size - LANES, moved, buffer_ref[cell + 1])
            return 0
        turns = (starts_ref[ranks, k] + window - 1) // window
        lax.fori_loop(1, turns, turn_body, 0)
        return 0
    lax.fori_loop(0, blocks, repair, 0)

    for d in range(ranks):
        for t in range(tiles):
            out_ref[d, :, t * LANES:(t + 1) * LANES] = buffer_ref[d * stride + t][0:4]

def pack(starts, coordinates, slot, place, ranks, width, window, unroll=4):
    blocks, _, rows = place.shape
    tiles = width // LANES
    vm = pl.BlockSpec(memory_space=pltpu.VMEM)
    return pl.pallas_call(
        functools.partial(pack_kernel, ranks=ranks, window=window, tiles=tiles, unroll=unroll),
        in_specs=[pl.BlockSpec(memory_space=pltpu.SMEM), vm, vm, vm],
        out_specs=vm,
        out_shape=jax.ShapeDtypeStruct((ranks, 4, width), jnp.float32),
        scratch_shapes=[pltpu.VMEM((ranks * (tiles + 2), 8, LANES), jnp.float32)],
        name="pack",
    )(starts, coordinates, slot, place)

def unpack_kernel(starts_ref, values_ref, place_ref, out_ref, *, ranks, window, tiles, unroll):
    blocks, _, rows = place_ref.shape
    per_tile = LANES // window
    lane = lax.broadcasted_iota(jnp.int32, (4, LANES), 1)

    def gather(k, turn, exact):
        parts = []
        for q in range(ranks // per_tile):
            mixed = None
            for i in range(per_tile):
                d, at = q * per_tile + i, i * window
                start = starts_ref[d, k]
                if not exact:
                    length = starts_ref[d, k + 1] - start
                    start = start + jnp.minimum(turn * window, length)
                tile, low = lax.shift_right_logical(start, 7), start & (LANES - 1)
                first = pl.multiple_of(jnp.minimum(tile, tiles - 1) * LANES, LANES)
                second = pl.multiple_of(jnp.minimum(tile + 1, tiles - 1) * LANES, LANES)
                both = jnp.where(lane >= low, values_ref[d, :, pl.ds(first, LANES)], values_ref[d, :, pl.ds(second, LANES)])
                moved = pltpu.roll(both, (at - low) & (LANES - 1), 1)
                mixed = moved if mixed is None else jnp.where(lane >= at, moved, mixed)
            parts.append(mixed)
        grouped = jnp.concatenate(parts, axis=1)
        grouped = jnp.concatenate([grouped, jnp.zeros_like(grouped)], axis=0)
        hot = one_hot(place_ref[k], ranks, window, turn)
        return join_rows(jnp.dot(split_rows(grouped), hot, preferred_element_type=jnp.float32))[0:4]

    def main(g, _):
        for u in range(unroll):
            k = g * unroll + u
            out_ref[:, pl.ds(pl.multiple_of(k * rows, LANES), rows)] = gather(k, 0, True)
        return 0
    lax.fori_loop(0, blocks // unroll, main, 0)

    def repair(k, _):
        def turn_body(turn, _):
            at = pl.ds(pl.multiple_of(k * rows, LANES), rows)
            out_ref[:, at] = out_ref[:, at] + gather(k, turn, False)
            return 0
        turns = (starts_ref[ranks, k] + window - 1) // window
        lax.fori_loop(1, turns, turn_body, 0)
        return 0
    lax.fori_loop(0, blocks, repair, 0)

def unpack(starts, values, place, window, unroll=4):
    blocks, _, rows = place.shape
    ranks, _, width = values.shape
    vm = pl.BlockSpec(memory_space=pltpu.VMEM)
    return pl.pallas_call(
        functools.partial(unpack_kernel, ranks=ranks, window=window, tiles=width // LANES, unroll=unroll),
        in_specs=[pl.BlockSpec(memory_space=pltpu.SMEM), vm, vm],
        out_specs=vm,
        out_shape=jax.ShapeDtypeStruct((4, blocks * rows), jnp.float32),
        name="unpack",
    )(starts, values, place)

def local(fields, coordinates, element_rank, element_slot):
    ranks = lax.axis_size(("gx", "gy", "gz"))
    probes = element_slot.shape[0]
    capacity = 5 * probes // (4 * ranks)
    width = -(-capacity // LANES) * LANES
    rows = math.gcd(probes, 512)
    window = max(8, 2 * rows // ranks)
    target = element_rank.reshape(probes // rows, 1, rows)
    slot = element_slot.reshape(probes // rows, 1, rows)
    place, starts = count(target, ranks, window)
    send = pack(starts, coordinates, slot, place, ranks, width, window)
    arrived = lax.all_to_all(send, ("gx", "gy", "gz"), split_axis=0, concat_axis=0, tiled=True)
    values = evaluate(arrived, fields)
    returned = lax.all_to_all(values, ("gx", "gy", "gz"), split_axis=0, concat_axis=0, tiled=True)
    return unpack(starts, returned, place, window)


def solution(mesh):
    placed = (
        P(("gx", "gy", "gz"), None),
        P(None, ("gx", "gy", "gz")),
        P(("gx", "gy", "gz"), None),
        P(("gx", "gy", "gz")),
    )
    return jax.shard_map(
        local, mesh=mesh, in_specs=placed, out_specs=P(None, ("gx", "gy", "gz")), check_vma=False
    )
```

```python
import functools
import math

import jax
import jax.numpy as jnp
import numpy as np
from jax import lax
from jax.experimental import pallas as pl
from jax.experimental.pallas import tpu as pltpu
from jax.sharding import PartitionSpec as P

LANES = 128

gll_points = np.array([-1.0,-0.8717401485096066,-0.5917001814331423,-0.2092992179024789,0.2092992179024789,0.5917001814331423,0.8717401485096066,1.0])
gll_scale = np.array([1.0 / np.prod([gll_points[a] - gll_points[b] for b in range(8) if b != a]) for a in range(8)])

def lagrange_rows(coord, scale, node):
    weights = jnp.broadcast_to(scale, node.shape)
    for b in range(8):
        offset = coord - np.float32(gll_points[b])
        weights = weights * jnp.where(node == b, np.float32(1.0), offset)
    return weights

def evaluate_kernel(table_ref, probes_ref, samples_ref, *, step):
    cells = probes_ref.shape[0]
    elements = table_ref.shape[1] // 8
    node = lax.broadcasted_iota(jnp.int32, (8, step), 0)
    scale = jnp.full((8, step), gll_scale[0], jnp.float32)
    for a in range(1, 8):
        scale = jnp.where(node == a, np.float32(gll_scale[a]), scale)
    ids = lax.broadcasted_iota(jnp.int32, (elements, step), 0).astype(jnp.float32).astype(jnp.bfloat16)
    per_step = step // LANES
    for at in range(0, cells, per_step):
        block = jnp.concatenate([probes_ref[at + i] for i in range(per_step)], axis=1)
        weight_r = lagrange_rows(block[0:1], scale, node)
        weight_s = lagrange_rows(block[1:2], scale, node)
        weight_t = lagrange_rows(block[2:3], scale, node)
        slot = jnp.broadcast_to(block[3:4], (elements, step)).astype(jnp.bfloat16)
        mine = slot == ids
        right = []
        for c in range(8):
            w = jnp.broadcast_to(weight_t[c:c + 1], (elements, step)).astype(jnp.bfloat16)
            right.append(jnp.where(mine, w, jnp.zeros_like(w)))
        right = jnp.concatenate(right, axis=0)
        along_t = jnp.dot(table_ref[...], right, preferred_element_type=jnp.float32)
        out = []
        for f in range(4):
            acc = None
            for b in range(8):
                at_b = (f * 8 + b) * 8
                term = along_t[at_b:at_b + 8] * weight_s[b:b + 1]
                acc = term if acc is None else acc + term
            out.append(jnp.sum(acc * weight_r, axis=0, keepdims=True))
        out = jnp.concatenate(out, axis=0)
        for i in range(per_step):
            samples_ref[at + i] = out[:, i * LANES:(i + 1) * LANES]

def evaluate(probes, fields, parts=2, step=256):
    cells = probes.shape[0]
    elements = fields.shape[0]
    table = fields.reshape(elements, 4, 8, 8, 8).transpose(1, 3, 2, 4, 0).reshape(256, 8 * elements)
    spec = pl.BlockSpec((cells // parts, 4, LANES), lambda i: (i, 0, 0))
    n = cells * LANES
    return pl.pallas_call(
        functools.partial(evaluate_kernel, step=step),
        grid=(parts,),
        in_specs=[pl.BlockSpec((256, 8 * elements), lambda i: (0, 0)), spec],
        out_specs=spec,
        out_shape=jax.ShapeDtypeStruct(probes.shape, jnp.float32),
        cost_estimate=pl.CostEstimate(flops=2 * n * 256 * 8 * elements, bytes_accessed=8 * n * 4, transcendentals=0),
        name="evaluate",
    )(table, probes)

def split_rows(x):
    high = x.astype(jnp.bfloat16)
    rest = x - high.astype(jnp.float32)
    middle = rest.astype(jnp.bfloat16)
    low = (rest - middle.astype(jnp.float32)).astype(jnp.bfloat16)
    return jnp.concatenate([high, middle, low, jnp.zeros_like(low)], axis=0)

def join_rows(y):
    return y[0:8] + y[8:16] + y[16:24]

def ones_where(mask):
    return jnp.where(mask, jnp.ones(mask.shape, jnp.bfloat16), jnp.zeros(mask.shape, jnp.bfloat16))

def count_blocks(target_ref, place_ref, words_ref, picks_ref, sums_ref, ranks, tiles):
    blocks, _, rows = target_ref.shape
    ident = lax.broadcasted_iota(jnp.int32, (ranks, rows), 0)
    for k in range(blocks):
        mine = jnp.broadcast_to(target_ref[k], (ranks, rows)) == ident
        picks_ref[k * ranks:(k + 1) * ranks, :] = jnp.where(mine, 1.0, 0.0).astype(jnp.bfloat16)
    upper = lax.broadcasted_iota(jnp.int32, (rows, rows), 0) <= lax.broadcasted_iota(jnp.int32, (rows, rows), 1)
    upper = jnp.where(upper, 1.0, 0.0).astype(jnp.bfloat16)
    sums_ref[...] = jnp.dot(picks_ref[...], upper, preferred_element_type=jnp.float32)
    lane = lax.broadcasted_iota(jnp.int32, (ranks, LANES), 1)
    counts = jnp.zeros((ranks, LANES), jnp.float32)
    running = jnp.zeros((ranks, 1), jnp.float32)
    table = jnp.zeros((ranks, LANES), jnp.float32)
    for k in range(blocks):
        at = slice(k * ranks, (k + 1) * ranks)
        target = jnp.broadcast_to(target_ref[k], (ranks, rows))
        last = sums_ref[at, rows - 1:rows]
        before = jnp.where(ident < target, last, 0.0)
        placed = jnp.sum(jnp.where(target == ident, sums_ref[at, :], before), axis=0, keepdims=True) - 1.0
        place_ref[k:k + 1, :] = placed.astype(jnp.int32)
        table = jnp.where(lane == k, running, table)
        counts = jnp.where(lane == k, last, counts)
        running = running + last
    lower = lax.broadcasted_iota(jnp.int32, (ranks, ranks), 0) > lax.broadcasted_iota(jnp.int32, (ranks, ranks), 1)
    lower = jnp.where(lower, 1.0, 0.0).astype(jnp.bfloat16)
    high = jnp.floor(counts * 0.0625)
    parts = [jnp.dot(lower, c.astype(jnp.bfloat16), preferred_element_type=jnp.float32) for c in (high, counts - 16.0 * high)]
    offset = (16.0 * parts[0] + parts[1]).astype(jnp.int32)
    start = table.astype(jnp.int32)
    tile, low = lax.shift_right_logical(start, 7), start & (LANES - 1)
    rank = lax.broadcasted_iota(jnp.int32, (ranks, LANES), 0)
    send = ((rank * (tiles + 2) + tile) << 23) | (jnp.minimum(offset, rows - 1) << 14) | (low << 7) | ((low - offset) & (LANES - 1))
    cell = rank * tiles + jnp.minimum(tile, tiles - 1)
    take = (cell << 24) | (offset << 14) | (low << 7) | ((offset - low) & (LANES - 1))
    most = jnp.broadcast_to(jnp.max(counts, axis=0, keepdims=True).astype(jnp.int32), (8, LANES))
    words = jnp.concatenate([send, take, counts.astype(jnp.int32), most], axis=0)
    spare = -words.shape[0] % LANES
    words = jnp.concatenate([words, jnp.zeros((spare, LANES), jnp.int32)], axis=0)
    for c in range(0, words.shape[0], LANES):
        words_ref[:, c:c + LANES] = words[c:c + LANES, :].T[0:blocks]

def field(word, shift, mask):
    return lax.shift_right_logical(jnp.full((8, LANES), word, jnp.int32), shift) & mask

def window(lane, offset, pieces):
    mixed = pieces[-1]
    for i in range(len(pieces) - 2, -1, -1):
        mixed = jnp.where(lane + i * LANES >= offset, pieces[i], mixed)
    return mixed

def pack_kernel(target_ref, coordinates_ref, slot_ref, out_ref, place_ref, words_ref, picks_ref, sums_ref, buffer_ref, known_ref, semaphore, *, ranks, tiles, unroll):
    blocks, rows = place_ref.shape
    pieces = rows // LANES
    lane = lax.broadcasted_iota(jnp.int32, (8, LANES), 1)
    count_blocks(target_ref, place_ref, words_ref, picks_ref, sums_ref, ranks, tiles)
    copy = pltpu.make_async_copy(words_ref, known_ref, semaphore)
    copy.start()

    def clear(i, _):
        buffer_ref[i] = jnp.zeros((8, LANES), jnp.float32)
        return 0
    lax.fori_loop(0, ranks * (tiles + 2), clear, 0, unroll=16)
    copy.wait()
    across = lax.broadcasted_iota(jnp.int32, (rows, LANES), 1).astype(jnp.int16)

    def ordered(k, column):
        at = pl.ds(pl.multiple_of(k * rows, LANES), rows)
        payload = jnp.concatenate([coordinates_ref[:, at], slot_ref[k].astype(jnp.float32), jnp.zeros((4, rows), jnp.float32)], axis=0)
        column = jnp.broadcast_to(column, (rows, LANES)).astype(jnp.int16)
        hot = jnp.concatenate([ones_where(column == across + np.int16(i * LANES)) for i in range(pieces)], axis=1)
        block = join_rows(jnp.dot(split_rows(payload), hot, preferred_element_type=jnp.float32))
        return [block[:, i * LANES:(i + 1) * LANES] for i in range(pieces)]

    def main(g, _):
        columns = place_ref[pl.ds(pl.multiple_of(g * 8, 8), 8), :].T
        for u in range(8):
            k = g * 8 + u
            block = ordered(k, columns[:, u:u + 1])
            for r in range(0, ranks, unroll):
                moves = []
                for d in range(r, r + unroll):
                    word = known_ref[k, d]
                    moved = pltpu.roll(window(lane, field(word, 14, 511), block), word, 1)
                    cell = lax.shift_right_logical(word, 23)
                    moves.append((cell, moved, jnp.where(lane < field(word, 7, 127), buffer_ref[cell], moved)))
                for cell, moved, mixed in moves:
                    buffer_ref[cell] = mixed
                    buffer_ref[cell + 1] = moved
        return 0
    lax.fori_loop(0, blocks // 8, main, 0)

    def repair(k, _):
        @pl.when(known_ref[k, 3 * ranks] > LANES)
        def _():
            column = jnp.broadcast_to(place_ref[pl.ds(k, 1), :], (8, rows)).T[:, 0:1]
            block = ordered(k, column)
            for m in range(1, pieces):
                for d in range(ranks):
                    size = known_ref[k, 2 * ranks + d] - m * LANES
                    @pl.when(size > 0)
                    def _():
                        word = known_ref[k, d]
                        moved = pltpu.roll(window(lane, field(word, 14, 511), block[m:] + block[:1]), word, 1)
                        low = field(word, 7, 127)
                        high = low + jnp.minimum(size, LANES)
                        cell = lax.shift_right_logical(word, 23) + m
                        buffer_ref[cell] = jnp.where((lane >= low) & (lane < high), moved, buffer_ref[cell])
                        buffer_ref[cell + 1] = jnp.where(lane + LANES < high, moved, buffer_ref[cell + 1])
        return 0
    lax.fori_loop(0, blocks, repair, 0)

    for d in range(ranks):
        for t in range(tiles):
            out_ref[d, t] = buffer_ref[d * (tiles + 2) + t][0:4]

def pack(target, coordinates, slot, ranks, tiles, unroll=4):
    blocks, _, rows = target.shape
    table = (blocks, -(-(3 * ranks + 1) // LANES) * LANES)
    vm = pl.BlockSpec(memory_space=pltpu.VMEM)
    return pl.pallas_call(
        functools.partial(pack_kernel, ranks=ranks, tiles=tiles, unroll=unroll),
        in_specs=[vm] * 3,
        out_specs=(vm,) * 3,
        out_shape=(
            jax.ShapeDtypeStruct((ranks, tiles, 4, LANES), jnp.float32),
            jax.ShapeDtypeStruct((blocks, rows), jnp.int32),
            jax.ShapeDtypeStruct(table, jnp.int32),
        ),
        scratch_shapes=[
            pltpu.VMEM((blocks * ranks, rows), jnp.bfloat16),
            pltpu.VMEM((blocks * ranks, rows), jnp.float32),
            pltpu.VMEM((ranks * (tiles + 2), 8, LANES), jnp.float32),
            pltpu.SMEM(table, jnp.int32),
            pltpu.SemaphoreType.DMA,
        ],
        name="pack",
    )(target, coordinates, slot)

def unpack_kernel(known_ref, values_ref, place_ref, out_ref, held_ref, *, ranks, unroll):
    blocks, rows = place_ref.shape
    cells = values_ref.shape[0]
    pieces = rows // LANES
    lane = lax.broadcasted_iota(jnp.int32, (4, LANES), 1)
    down = lax.broadcasted_iota(jnp.int32, (rows, rows), 0).astype(jnp.int16)
    for i in range(cells):
        held_ref[i] = values_ref[i]
    held_ref[cells] = values_ref[0]

    def emit(k, row, whole):
        block = [jnp.zeros((4, LANES), jnp.float32)] * pieces
        for d in range(ranks):
            word = known_ref[k, ranks + d]
            cell = lax.shift_right_logical(word, 24)
            offset, low = field(word, 14, 1023)[0:4], field(word, 7, 127)[0:4]
            for m in range(pieces if whole else 1):
                at = [jnp.minimum(cell + m + i, cells) if m else cell + i for i in (0, 1)]
                moved = pltpu.roll(jnp.where(lane >= low, held_ref[at[0]], held_ref[at[1]]), word, 1)
                for i in range(m, pieces):
                    block[i] = jnp.where(lane + (i - m) * LANES >= offset, moved, block[i])
        block = jnp.concatenate(block, axis=1)
        block = jnp.concatenate([block, jnp.zeros_like(block)], axis=0)
        at = pl.ds(pl.multiple_of(k * rows, LANES), rows)
        hot = ones_where(jnp.broadcast_to(row, (rows, rows)).astype(jnp.int16) == down)
        out_ref[:, at] = join_rows(jnp.dot(split_rows(block), hot, preferred_element_type=jnp.float32))[0:4]

    def main(g, _):
        for u in range(unroll):
            k = g * unroll + u
            emit(k, place_ref[pl.ds(k, 1), :], False)
        return 0
    lax.fori_loop(0, blocks // unroll, main, 0)

    def repair(k, _):
        @pl.when(known_ref[k, 3 * ranks] > LANES)
        def _():
            emit(k, place_ref[pl.ds(k, 1), :], True)
        return 0
    lax.fori_loop(0, blocks, repair, 0)

def unpack(words, values, place, unroll=8):
    blocks, rows = place.shape
    ranks, tiles = values.shape[:2]
    vm = pl.BlockSpec(memory_space=pltpu.VMEM)
    return pl.pallas_call(
        functools.partial(unpack_kernel, ranks=ranks, unroll=unroll),
        in_specs=[pl.BlockSpec(memory_space=pltpu.SMEM), vm, vm],
        out_specs=vm,
        out_shape=jax.ShapeDtypeStruct((4, blocks * rows), jnp.float32),
        scratch_shapes=[pltpu.VMEM((ranks * tiles + 1, 4, LANES), jnp.float32)],
        name="unpack",
    )(words, values.reshape(ranks * tiles, 4, LANES), place)

def local(fields, coordinates, element_rank, element_slot):
    ranks = lax.axis_size(("gx", "gy", "gz"))
    probes = element_slot.shape[0]
    capacity = 5 * probes // (4 * ranks)
    tiles = -(-capacity // LANES)
    rows = math.gcd(probes, 512)
    target = element_rank.reshape(probes // rows, 1, rows)
    slot = element_slot.reshape(probes // rows, 1, rows)
    send, place, words = pack(target, coordinates, slot, ranks, tiles)
    arrived = lax.all_to_all(send, ("gx", "gy", "gz"), split_axis=0, concat_axis=0, tiled=True)
    values = evaluate(arrived.reshape(ranks * tiles, 4, LANES), fields).reshape(ranks, tiles, 4, LANES)
    returned = lax.all_to_all(values, ("gx", "gy", "gz"), split_axis=0, concat_axis=0, tiled=True)
    return unpack(words, returned, place)


def solution(mesh):
    placed = (
        P(("gx", "gy", "gz"), None),
        P(None, ("gx", "gy", "gz")),
        P(("gx", "gy", "gz"), None),
        P(("gx", "gy", "gz")),
    )
    return jax.shard_map(
        local, mesh=mesh, in_specs=placed, out_specs=P(None, ("gx", "gy", "gz")), check_vma=False
    )
```

```python
import functools
import math

import jax
import jax.numpy as jnp
import numpy as np
from jax import lax
from jax.experimental import pallas as pl
from jax.experimental.pallas import tpu as pltpu
from jax.sharding import PartitionSpec as P

LANES = 128

gll_points = np.array([-1.0,-0.8717401485096066,-0.5917001814331423,-0.2092992179024789,0.2092992179024789,0.5917001814331423,0.8717401485096066,1.0])
gll_scale = np.array([1.0 / np.prod([gll_points[a] - gll_points[b] for b in range(8) if b != a]) for a in range(8)])

def lagrange_rows(coord, scale, node):
    weights = jnp.broadcast_to(scale, node.shape)
    for b in range(8):
        offset = coord - np.float32(gll_points[b])
        weights = weights * jnp.where(node == b, np.float32(1.0), offset)
    return weights

def evaluate_kernel(table_ref, probes_ref, samples_ref, *, step):
    cells = probes_ref.shape[0]
    elements = table_ref.shape[1] // 8
    node = lax.broadcasted_iota(jnp.int32, (8, step), 0)
    scale = jnp.full((8, step), gll_scale[0], jnp.float32)
    for a in range(1, 8):
        scale = jnp.where(node == a, np.float32(gll_scale[a]), scale)
    ids = lax.broadcasted_iota(jnp.int32, (elements, step), 0).astype(jnp.float32).astype(jnp.bfloat16)
    per_step = step // LANES
    for at in range(0, cells, per_step):
        block = jnp.concatenate([probes_ref[at + i] for i in range(per_step)], axis=1)
        weight_r = lagrange_rows(block[0:1], scale, node)
        weight_s = lagrange_rows(block[1:2], scale, node)
        weight_t = lagrange_rows(block[2:3], scale, node)
        slot = jnp.broadcast_to(block[3:4], (elements, step)).astype(jnp.bfloat16)
        mine = slot == ids
        right = []
        for c in range(8):
            w = jnp.broadcast_to(weight_t[c:c + 1], (elements, step)).astype(jnp.bfloat16)
            right.append(jnp.where(mine, w, jnp.zeros_like(w)))
        right = jnp.concatenate(right, axis=0)
        along_t = jnp.dot(table_ref[...], right, preferred_element_type=jnp.float32)
        out = []
        for f in range(4):
            acc = None
            for b in range(8):
                at_b = (f * 8 + b) * 8
                term = along_t[at_b:at_b + 8] * weight_s[b:b + 1]
                acc = term if acc is None else acc + term
            out.append(jnp.sum(acc * weight_r, axis=0, keepdims=True))
        out = jnp.concatenate(out, axis=0)
        for i in range(per_step):
            samples_ref[at + i] = out[:, i * LANES:(i + 1) * LANES]

def evaluate(probes, fields, parts=2, step=256):
    cells = probes.shape[0]
    elements = fields.shape[0]
    table = fields.reshape(elements, 4, 8, 8, 8).transpose(1, 3, 2, 4, 0).reshape(256, 8 * elements)
    spec = pl.BlockSpec((cells // parts, 4, LANES), lambda i: (i, 0, 0))
    n = cells * LANES
    return pl.pallas_call(
        functools.partial(evaluate_kernel, step=step),
        grid=(parts,),
        in_specs=[pl.BlockSpec((256, 8 * elements), lambda i: (0, 0)), spec],
        out_specs=spec,
        out_shape=jax.ShapeDtypeStruct(probes.shape, jnp.float32),
        cost_estimate=pl.CostEstimate(flops=2 * n * 256 * 8 * elements, bytes_accessed=8 * n * 4, transcendentals=0),
        compiler_params=pltpu.CompilerParams(vmem_limit_bytes=16 << 20),
        name="evaluate",
    )(table, probes)

def split_rows(x):
    high = x.astype(jnp.bfloat16)
    rest = x - high.astype(jnp.float32)
    middle = rest.astype(jnp.bfloat16)
    low = (rest - middle.astype(jnp.float32)).astype(jnp.bfloat16)
    return jnp.concatenate([high, middle, low, jnp.zeros_like(low)], axis=0)

def join_rows(y):
    return y[0:8] + y[8:16] + y[16:24]

def ones_where(mask):
    return jnp.where(mask, jnp.ones(mask.shape, jnp.bfloat16), jnp.zeros(mask.shape, jnp.bfloat16))

def count_blocks(target_ref, place_ref, words_ref, picks_ref, sums_ref, ranks, tiles):
    blocks, _, rows = target_ref.shape
    ident = lax.broadcasted_iota(jnp.int32, (ranks, rows), 0)
    for k in range(blocks):
        mine = jnp.broadcast_to(target_ref[k], (ranks, rows)) == ident
        picks_ref[k * ranks:(k + 1) * ranks, :] = jnp.where(mine, 1.0, 0.0).astype(jnp.bfloat16)
    upper = lax.broadcasted_iota(jnp.int32, (rows, rows), 0) <= lax.broadcasted_iota(jnp.int32, (rows, rows), 1)
    upper = jnp.where(upper, 1.0, 0.0).astype(jnp.bfloat16)
    sums_ref[...] = jnp.dot(picks_ref[...], upper, preferred_element_type=jnp.float32)
    lane = lax.broadcasted_iota(jnp.int32, (ranks, LANES), 1)
    counts = jnp.zeros((ranks, LANES), jnp.float32)
    running = jnp.zeros((ranks, 1), jnp.float32)
    table = jnp.zeros((ranks, LANES), jnp.float32)
    for k in range(blocks):
        at = slice(k * ranks, (k + 1) * ranks)
        target = jnp.broadcast_to(target_ref[k], (ranks, rows))
        last = sums_ref[at, rows - 1:rows]
        before = jnp.where(ident < target, last, 0.0)
        placed = jnp.sum(jnp.where(target == ident, sums_ref[at, :], before), axis=0, keepdims=True) - 1.0
        place_ref[k:k + 1, :] = placed.astype(jnp.int32)
        table = jnp.where(lane == k, running, table)
        counts = jnp.where(lane == k, last, counts)
        running = running + last
    lower = lax.broadcasted_iota(jnp.int32, (ranks, ranks), 0) > lax.broadcasted_iota(jnp.int32, (ranks, ranks), 1)
    lower = jnp.where(lower, 1.0, 0.0).astype(jnp.bfloat16)
    high = jnp.floor(counts * 0.0625)
    parts = [jnp.dot(lower, c.astype(jnp.bfloat16), preferred_element_type=jnp.float32) for c in (high, counts - 16.0 * high)]
    offset = (16.0 * parts[0] + parts[1]).astype(jnp.int32)
    start = table.astype(jnp.int32)
    tile, low = lax.shift_right_logical(start, 7), start & (LANES - 1)
    rank = lax.broadcasted_iota(jnp.int32, (ranks, LANES), 0)
    send = ((rank * (tiles + 2) + tile) << 23) | (jnp.minimum(offset, rows - 1) << 14) | (low << 7) | ((low - offset) & (LANES - 1))
    cell = rank * tiles + jnp.minimum(tile, tiles - 1)
    take = (cell << 24) | (offset << 14) | (low << 7) | ((offset - low) & (LANES - 1))
    most = jnp.max(counts, axis=0, keepdims=True)
    peak = jnp.broadcast_to(jnp.max(most, axis=1, keepdims=True), most.shape)
    most = jnp.concatenate([most, peak, jnp.zeros((6, LANES), jnp.float32)], axis=0).astype(jnp.int32)
    words = jnp.concatenate([send, take, counts.astype(jnp.int32), most], axis=0)
    spare = -words.shape[0] % LANES
    words = jnp.concatenate([words, jnp.zeros((spare, LANES), jnp.int32)], axis=0)
    for c in range(0, words.shape[0], LANES):
        words_ref[:, c:c + LANES] = words[c:c + LANES, :].T[0:blocks]

def reach(lane, shift, i=0):
    return ((lane + i * LANES) << shift) | ((1 << shift) - 1)

def window(lane, offset, pieces):
    mixed = pieces[-1]
    for i in range(len(pieces) - 2, -1, -1):
        mixed = jnp.where(reach(lane, 14, i) >= offset, pieces[i], mixed)
    return mixed

def pack_kernel(target_hbm, coordinates_hbm, slot_hbm, out_ref, place_ref, words_ref, target_ref, coordinates_ref, slot_ref, picks_ref, sums_ref, buffer_ref, known_ref, semaphores, *, ranks, tiles, unroll):
    blocks, rows = place_ref.shape
    pieces = rows // LANES
    lane = lax.broadcasted_iota(jnp.int32, (8, LANES), 1)
    fetches = [
        pltpu.make_async_copy(target_hbm, target_ref, semaphores.at[0]),
        pltpu.make_async_copy(coordinates_hbm, coordinates_ref, semaphores.at[1]),
        pltpu.make_async_copy(slot_hbm, slot_ref, semaphores.at[2]),
    ]
    for fetch in fetches:
        fetch.start()
    fetches[0].wait()
    count_blocks(target_ref, place_ref, words_ref, picks_ref, sums_ref, ranks, tiles)
    copy = pltpu.make_async_copy(words_ref, known_ref, semaphores.at[3])
    copy.start()

    def clear(i, _):
        buffer_ref[i] = jnp.zeros((8, LANES), jnp.float32)
        return 0
    lax.fori_loop(0, ranks * (tiles + 2), clear, 0, unroll=16)
    copy.wait()
    for fetch in fetches[1:]:
        fetch.wait()
    down = lax.broadcasted_iota(jnp.int32, (rows, rows), 0).astype(jnp.int16)

    def ordered(k):
        at = pl.ds(pl.multiple_of(k * rows, LANES), rows)
        payload = jnp.concatenate([coordinates_ref[:, at], slot_ref[k].astype(jnp.float32), jnp.zeros((4, rows), jnp.float32)], axis=0)
        hot = ones_where(jnp.broadcast_to(place_ref[pl.ds(k, 1), :], (rows, rows)).astype(jnp.int16) == down)
        block = join_rows(lax.dot_general(split_rows(payload), hot, (((1,), (1,)), ((), ())), preferred_element_type=jnp.float32))
        return [block[:, i * LANES:(i + 1) * LANES] for i in range(pieces)]

    def main(g, _):
        for u in range(8):
            k = g * 8 + u
            block = ordered(k)
            for r in range(0, ranks, unroll):
                moves = []
                for d in range(r, r + unroll):
                    word = known_ref[k, d]
                    wide = jnp.full((8, LANES), word, jnp.int32)
                    moved = pltpu.roll(window(lane, wide & ((1 << 23) - 1), block), word, 1)
                    moves.append((lax.shift_right_logical(word, 23), moved, reach(lane, 7) >= (wide & ((1 << 14) - 1))))
                for cell, moved, mask in moves:
                    pltpu.store(buffer_ref.at[cell], moved, mask=mask)
                    buffer_ref[cell + 1] = moved
        return 0
    lax.fori_loop(0, blocks // 8, main, 0)

    def repair(k, _):
        @pl.when(known_ref[k, 3 * ranks] > LANES)
        def _():
            block = ordered(k)
            for m in range(1, pieces):
                for d in range(ranks):
                    size = known_ref[k, 2 * ranks + d] - m * LANES
                    @pl.when(size > 0)
                    def _():
                        word = known_ref[k, d]
                        moved = pltpu.roll(window(lane, word & ((1 << 23) - 1), block[m:] + block[:1]), word, 1)
                        low = lax.shift_right_logical(word, 7) & (LANES - 1)
                        high = low + jnp.minimum(size, LANES)
                        cell = lax.shift_right_logical(word, 23) + m
                        buffer_ref[cell] = jnp.where((lane >= low) & (lane < high), moved, buffer_ref[cell])
                        buffer_ref[cell + 1] = jnp.where(lane + LANES < high, moved, buffer_ref[cell + 1])
        return 0

    @pl.when(known_ref[0, 3 * ranks + 1] > LANES)
    def _():
        lax.fori_loop(0, blocks, repair, 0)

    for d in range(ranks):
        for t in range(tiles):
            out_ref[d, t] = buffer_ref[d * (tiles + 2) + t][0:4]

def pack(target, coordinates, slot, ranks, tiles, unroll=4):
    blocks, _, rows = target.shape
    table = (blocks, -(-(3 * ranks + 2) // LANES) * LANES)
    vm = pl.BlockSpec(memory_space=pltpu.VMEM)
    return pl.pallas_call(
        functools.partial(pack_kernel, ranks=ranks, tiles=tiles, unroll=unroll),
        in_specs=[pl.BlockSpec(memory_space=pltpu.HBM)] * 3,
        out_specs=(vm,) * 3,
        out_shape=(
            jax.ShapeDtypeStruct((ranks, tiles, 4, LANES), jnp.float32),
            jax.ShapeDtypeStruct((blocks, rows), jnp.int32),
            jax.ShapeDtypeStruct(table, jnp.int32),
        ),
        scratch_shapes=[
            pltpu.VMEM(target.shape, jnp.int32),
            pltpu.VMEM(coordinates.shape, jnp.float32),
            pltpu.VMEM(slot.shape, jnp.int32),
            pltpu.VMEM((blocks * ranks, rows), jnp.bfloat16),
            pltpu.VMEM((blocks * ranks, rows), jnp.float32),
            pltpu.VMEM((ranks * (tiles + 2), 8, LANES), jnp.float32),
            pltpu.SMEM(table, jnp.int32),
            pltpu.SemaphoreType.DMA((4,)),
        ],
        compiler_params=pltpu.CompilerParams(vmem_limit_bytes=60 << 20),
        name="pack",
    )(target, coordinates, slot)

def unpack_kernel(known_ref, values_ref, place_ref, out_ref, held_ref, *, ranks, unroll):
    blocks, rows = place_ref.shape
    cells = values_ref.shape[0]
    pieces = rows // LANES
    lane = lax.broadcasted_iota(jnp.int32, (4, LANES), 1)
    down = lax.broadcasted_iota(jnp.int32, (rows, rows), 0).astype(jnp.int16)
    for i in range(cells):
        held_ref[i] = values_ref[i]
    held_ref[cells] = values_ref[0]

    def emit(k, row, whole):
        block = [jnp.zeros((4, LANES), jnp.float32)] * pieces
        for d in range(ranks):
            word = known_ref[k, ranks + d]
            cell = lax.shift_right_logical(word, 24)
            wide = jnp.full((4, LANES), word, jnp.int32)
            offset, low = wide & ((1 << 24) - 1), wide & ((1 << 14) - 1)
            for m in range(pieces if whole else 1):
                at = [jnp.minimum(cell + m + i, cells) if m else cell + i for i in (0, 1)]
                moved = pltpu.roll(jnp.where(reach(lane, 7) >= low, held_ref[at[0]], held_ref[at[1]]), word, 1)
                for i in range(m, pieces):
                    block[i] = jnp.where(reach(lane, 14, i - m) >= offset, moved, block[i])
        block = jnp.concatenate(block, axis=1)
        block = jnp.concatenate([block, jnp.zeros_like(block)], axis=0)
        at = pl.ds(pl.multiple_of(k * rows, LANES), rows)
        hot = ones_where(jnp.broadcast_to(row, (rows, rows)).astype(jnp.int16) == down)
        out_ref[:, at] = join_rows(jnp.dot(split_rows(block), hot, preferred_element_type=jnp.float32))[0:4]

    def main(g, _):
        for u in range(unroll):
            k = g * unroll + u
            emit(k, place_ref[pl.ds(k, 1), :], False)
        return 0
    lax.fori_loop(0, blocks // unroll, main, 0)

    def repair(k, _):
        @pl.when(known_ref[k, 3 * ranks] > LANES)
        def _():
            emit(k, place_ref[pl.ds(k, 1), :], True)
        return 0

    @pl.when(known_ref[0, 3 * ranks + 1] > LANES)
    def _():
        lax.fori_loop(0, blocks, repair, 0)

def unpack(words, values, place, unroll=8):
    blocks, rows = place.shape
    ranks, tiles = values.shape[:2]
    vm = pl.BlockSpec(memory_space=pltpu.VMEM)
    return pl.pallas_call(
        functools.partial(unpack_kernel, ranks=ranks, unroll=unroll),
        in_specs=[pl.BlockSpec(memory_space=pltpu.SMEM), vm, vm],
        out_specs=vm,
        out_shape=jax.ShapeDtypeStruct((4, blocks * rows), jnp.float32),
        scratch_shapes=[pltpu.VMEM((ranks * tiles + 1, 4, LANES), jnp.float32)],
        compiler_params=pltpu.CompilerParams(vmem_limit_bytes=8 << 20),
        name="unpack",
    )(words, values.reshape(ranks * tiles, 4, LANES), place)

def local(fields, coordinates, element_rank, element_slot):
    ranks = lax.axis_size(("gx", "gy", "gz"))
    probes = element_slot.shape[0]
    capacity = 5 * probes // (4 * ranks)
    tiles = -(-capacity // LANES)
    rows = math.gcd(probes, 512)
    target = element_rank.reshape(probes // rows, 1, rows)
    slot = element_slot.reshape(probes // rows, 1, rows)
    send, place, words = pack(target, coordinates, slot, ranks, tiles)
    arrived = lax.all_to_all(send, ("gx", "gy", "gz"), split_axis=0, concat_axis=0, tiled=True)
    values = evaluate(arrived.reshape(ranks * tiles, 4, LANES), fields).reshape(ranks, tiles, 4, LANES)
    returned = lax.all_to_all(values, ("gx", "gy", "gz"), split_axis=0, concat_axis=0, tiled=True)
    return unpack(words, returned, place)


def solution(mesh):
    placed = (
        P(("gx", "gy", "gz"), None),
        P(None, ("gx", "gy", "gz")),
        P(("gx", "gy", "gz"), None),
        P(("gx", "gy", "gz")),
    )
    return jax.shard_map(
        local, mesh=mesh, in_specs=placed, out_specs=P(None, ("gx", "gy", "gz")), check_vma=False
    )
```

```python
import functools
import math

import jax
import jax.numpy as jnp
import numpy as np
from jax import lax
from jax.experimental import pallas as pl
from jax.experimental.pallas import tpu as pltpu
from jax.sharding import PartitionSpec as P

LANES = 128

gll_points = np.array([-1.0,-0.8717401485096066,-0.5917001814331423,-0.2092992179024789,0.2092992179024789,0.5917001814331423,0.8717401485096066,1.0])
gll_scale = np.array([1.0 / np.prod([gll_points[a] - gll_points[b] for b in range(8) if b != a]) for a in range(8)])

def lagrange_rows(coord, scale, node):
    weights = jnp.broadcast_to(scale, node.shape)
    for b in range(8):
        offset = coord - np.float32(gll_points[b])
        weights = weights * jnp.where(node == b, np.float32(1.0), offset)
    return weights

def evaluate_kernel(table_ref, probes_ref, samples_ref, *, step):
    cells = probes_ref.shape[0]
    elements = table_ref.shape[1] // 8
    node = lax.broadcasted_iota(jnp.int32, (8, step), 0)
    scale = jnp.full((8, step), gll_scale[0], jnp.float32)
    for a in range(1, 8):
        scale = jnp.where(node == a, np.float32(gll_scale[a]), scale)
    ids = lax.broadcasted_iota(jnp.int32, (elements, step), 0).astype(jnp.float32).astype(jnp.bfloat16)
    per_step = step // LANES
    for at in range(0, cells, per_step):
        block = jnp.concatenate([probes_ref[at + i] for i in range(per_step)], axis=1)
        weight_r = lagrange_rows(block[0:1], scale, node)
        weight_s = lagrange_rows(block[1:2], scale, node)
        weight_t = lagrange_rows(block[2:3], scale, node)
        slot = jnp.broadcast_to(block[3:4], (elements, step)).astype(jnp.bfloat16)
        mine = slot == ids
        right = []
        for c in range(8):
            w = jnp.broadcast_to(weight_t[c:c + 1], (elements, step)).astype(jnp.bfloat16)
            right.append(jnp.where(mine, w, jnp.zeros_like(w)))
        right = jnp.concatenate(right, axis=0)
        along_t = jnp.dot(table_ref[...], right, preferred_element_type=jnp.float32)
        out = []
        for f in range(4):
            acc = None
            for b in range(8):
                at_b = (f * 8 + b) * 8
                term = along_t[at_b:at_b + 8] * weight_s[b:b + 1]
                acc = term if acc is None else acc + term
            out.append(jnp.sum(acc * weight_r, axis=0, keepdims=True))
        out = jnp.concatenate(out, axis=0)
        for i in range(per_step):
            samples_ref[at + i] = out[:, i * LANES:(i + 1) * LANES]

def evaluate(probes, fields, parts=2, step=256):
    cells = probes.shape[0]
    elements = fields.shape[0]
    table = fields.reshape(elements, 4, 8, 8, 8).transpose(1, 3, 2, 4, 0).reshape(256, 8 * elements)
    spec = pl.BlockSpec((cells // parts, 4, LANES), lambda i: (i, 0, 0))
    n = cells * LANES
    return pl.pallas_call(
        functools.partial(evaluate_kernel, step=step),
        grid=(parts,),
        in_specs=[pl.BlockSpec((256, 8 * elements), lambda i: (0, 0)), spec],
        out_specs=spec,
        out_shape=jax.ShapeDtypeStruct(probes.shape, jnp.float32),
        cost_estimate=pl.CostEstimate(flops=2 * n * 256 * 8 * elements, bytes_accessed=8 * n * 4, transcendentals=0),
        compiler_params=pltpu.CompilerParams(vmem_limit_bytes=16 << 20),
        name="evaluate",
    )(table, probes)

def split_rows(x):
    high = x.astype(jnp.bfloat16)
    rest = x - high.astype(jnp.float32)
    middle = rest.astype(jnp.bfloat16)
    low = (rest - middle.astype(jnp.float32)).astype(jnp.bfloat16)
    return jnp.concatenate([high, middle, low, jnp.zeros_like(low)], axis=0)

def join_rows(y):
    return y[0:8] + y[8:16] + y[16:24]

def ones_where(mask):
    return jnp.where(mask, jnp.ones(mask.shape, jnp.bfloat16), jnp.zeros(mask.shape, jnp.bfloat16))

def count_blocks(target_ref, place_ref, words_ref, picks_ref, sums_ref, ranks, tiles):
    blocks, _, rows = target_ref.shape
    ident = lax.broadcasted_iota(jnp.int32, (ranks, rows), 0)
    for k in range(blocks):
        mine = jnp.broadcast_to(target_ref[k], (ranks, rows)) == ident
        picks_ref[k * ranks:(k + 1) * ranks, :] = jnp.where(mine, 1.0, 0.0).astype(jnp.bfloat16)
    upper = lax.broadcasted_iota(jnp.int32, (rows, rows), 0) <= lax.broadcasted_iota(jnp.int32, (rows, rows), 1)
    upper = jnp.where(upper, 1.0, 0.0).astype(jnp.bfloat16)
    sums_ref[...] = jnp.dot(picks_ref[...], upper, preferred_element_type=jnp.float32)
    lane = lax.broadcasted_iota(jnp.int32, (ranks, LANES), 1)
    counts = jnp.zeros((ranks, LANES), jnp.float32)
    running = jnp.zeros((ranks, 1), jnp.float32)
    table = jnp.zeros((ranks, LANES), jnp.float32)
    for k in range(blocks):
        at = slice(k * ranks, (k + 1) * ranks)
        target = jnp.broadcast_to(target_ref[k], (ranks, rows))
        last = sums_ref[at, rows - 1:rows]
        before = jnp.where(ident < target, last, 0.0)
        placed = jnp.sum(jnp.where(target == ident, sums_ref[at, :], before), axis=0, keepdims=True) - 1.0
        place_ref[k:k + 1, :] = placed.astype(jnp.int32)
        table = jnp.where(lane == k, running, table)
        counts = jnp.where(lane == k, last, counts)
        running = running + last
    lower = lax.broadcasted_iota(jnp.int32, (ranks, ranks), 0) > lax.broadcasted_iota(jnp.int32, (ranks, ranks), 1)
    lower = jnp.where(lower, 1.0, 0.0).astype(jnp.bfloat16)
    high = jnp.floor(counts * 0.0625)
    parts = [jnp.dot(lower, c.astype(jnp.bfloat16), preferred_element_type=jnp.float32) for c in (high, counts - 16.0 * high)]
    offset = (16.0 * parts[0] + parts[1]).astype(jnp.int32)
    start = table.astype(jnp.int32)
    tile, low = lax.shift_right_logical(start, 7), start & (LANES - 1)
    rank = lax.broadcasted_iota(jnp.int32, (ranks, LANES), 0)
    send = ((rank * (tiles + 2) + tile) << 23) | (jnp.minimum(offset, rows - 1) << 14) | (low << 7) | ((low - offset) & (LANES - 1))
    cell = rank * tiles + jnp.minimum(tile, tiles - 1)
    take = (cell << 24) | (offset << 14) | (low << 7) | ((offset - low) & (LANES - 1))
    most = jnp.max(counts, axis=0, keepdims=True)
    peak = jnp.broadcast_to(jnp.max(most, axis=1, keepdims=True), most.shape)
    most = jnp.concatenate([most, peak, jnp.zeros((6, LANES), jnp.float32)], axis=0).astype(jnp.int32)
    words = jnp.concatenate([send, take, counts.astype(jnp.int32), most], axis=0)
    spare = -words.shape[0] % LANES
    words = jnp.concatenate([words, jnp.zeros((spare, LANES), jnp.int32)], axis=0)
    for c in range(0, words.shape[0], LANES):
        words_ref[:, c:c + LANES] = words[c:c + LANES, :].T[0:blocks]

def span_of(blocks, ranks):
    return math.gcd(blocks, max(1, 1024 // ranks))

def for_blocks(blocks, span, body):
    if span == blocks:
        body(0, 0)
    else:
        lax.fori_loop(0, blocks // span, body, 0)

def reach(lane, shift, i=0):
    return ((lane + i * LANES) << shift) | ((1 << shift) - 1)

def window(lane, offset, pieces):
    mixed = pieces[-1]
    for i in range(len(pieces) - 2, -1, -1):
        mixed = jnp.where(reach(lane, 14, i) >= offset, pieces[i], mixed)
    return mixed

def pack_kernel(target_hbm, coordinates_hbm, slot_hbm, out_ref, place_ref, words_ref, target_ref, coordinates_ref, slot_ref, picks_ref, sums_ref, buffer_ref, known_ref, semaphores, *, ranks, tiles, unroll, span):
    blocks, rows = place_ref.shape
    pieces = rows // LANES
    lane = lax.broadcasted_iota(jnp.int32, (8, LANES), 1)
    fetches = [
        pltpu.make_async_copy(target_hbm, target_ref, semaphores.at[0]),
        pltpu.make_async_copy(coordinates_hbm, coordinates_ref, semaphores.at[1]),
        pltpu.make_async_copy(slot_hbm, slot_ref, semaphores.at[2]),
    ]
    for fetch in fetches:
        fetch.start()
    fetches[0].wait()
    count_blocks(target_ref, place_ref, words_ref, picks_ref, sums_ref, ranks, tiles)
    copy = pltpu.make_async_copy(words_ref, known_ref, semaphores.at[3])
    copy.start()

    def clear(i, _):
        buffer_ref[i] = jnp.zeros((8, LANES), jnp.float32)
        return 0
    lax.fori_loop(0, ranks * (tiles + 2), clear, 0, unroll=16)
    copy.wait()
    for fetch in fetches[1:]:
        fetch.wait()
    down = lax.broadcasted_iota(jnp.int32, (rows, rows), 0).astype(jnp.int16)

    def ordered(k):
        at = pl.ds(pl.multiple_of(k * rows, LANES), rows)
        payload = jnp.concatenate([coordinates_ref[:, at], slot_ref[k].astype(jnp.float32), jnp.zeros((4, rows), jnp.float32)], axis=0)
        hot = ones_where(jnp.broadcast_to(place_ref[pl.ds(k, 1), :], (rows, rows)).astype(jnp.int16) == down)
        block = join_rows(lax.dot_general(split_rows(payload), hot, (((1,), (1,)), ((), ())), preferred_element_type=jnp.float32))
        return [block[:, i * LANES:(i + 1) * LANES] for i in range(pieces)]

    def spread(k, block):
        for r in range(0, ranks, unroll):
            moves = []
            for d in range(r, r + unroll):
                word = known_ref[k, d]
                wide = jnp.full((8, LANES), word, jnp.int32)
                moved = pltpu.roll(window(lane, wide & ((1 << 23) - 1), block), word, 1)
                moves.append((lax.shift_right_logical(word, 23), moved, reach(lane, 7) >= (wide & ((1 << 14) - 1))))
            for cell, moved, mask in moves:
                pltpu.store(buffer_ref.at[cell], moved, mask=mask)
                buffer_ref[cell + 1] = moved

    def main(g, _):
        for u in range(span):
            k = g * span + u
            spread(k, ordered(k))
        return 0
    for_blocks(blocks, span, main)

    def repair(k, _):
        @pl.when(known_ref[k, 3 * ranks] > LANES)
        def _():
            block = ordered(k)
            for m in range(1, pieces):
                for d in range(ranks):
                    size = known_ref[k, 2 * ranks + d] - m * LANES
                    @pl.when(size > 0)
                    def _():
                        word = known_ref[k, d]
                        moved = pltpu.roll(window(lane, word & ((1 << 23) - 1), block[m:] + block[:1]), word, 1)
                        low = lax.shift_right_logical(word, 7) & (LANES - 1)
                        high = low + jnp.minimum(size, LANES)
                        cell = lax.shift_right_logical(word, 23) + m
                        buffer_ref[cell] = jnp.where((lane >= low) & (lane < high), moved, buffer_ref[cell])
                        buffer_ref[cell + 1] = jnp.where(lane + LANES < high, moved, buffer_ref[cell + 1])
        return 0

    @pl.when(known_ref[0, 3 * ranks + 1] > LANES)
    def _():
        lax.fori_loop(0, blocks, repair, 0)

    for d in range(ranks):
        for t in range(tiles):
            out_ref[d, t] = buffer_ref[d * (tiles + 2) + t][0:4]

def pack(target, coordinates, slot, ranks, tiles, unroll=4):
    blocks, _, rows = target.shape
    table = (blocks, -(-(3 * ranks + 2) // LANES) * LANES)
    vm = pl.BlockSpec(memory_space=pltpu.VMEM)
    return pl.pallas_call(
        functools.partial(pack_kernel, ranks=ranks, tiles=tiles, unroll=unroll, span=span_of(blocks, ranks)),
        in_specs=[pl.BlockSpec(memory_space=pltpu.HBM)] * 3,
        out_specs=(vm,) * 3,
        out_shape=(
            jax.ShapeDtypeStruct((ranks, tiles, 4, LANES), jnp.float32),
            jax.ShapeDtypeStruct((blocks, rows), jnp.int32),
            jax.ShapeDtypeStruct(table, jnp.int32),
        ),
        scratch_shapes=[
            pltpu.VMEM(target.shape, jnp.int32),
            pltpu.VMEM(coordinates.shape, jnp.float32),
            pltpu.VMEM(slot.shape, jnp.int32),
            pltpu.VMEM((blocks * ranks, rows), jnp.bfloat16),
            pltpu.VMEM((blocks * ranks, rows), jnp.float32),
            pltpu.VMEM((ranks * (tiles + 2), 8, LANES), jnp.float32),
            pltpu.SMEM(table, jnp.int32),
            pltpu.SemaphoreType.DMA((4,)),
        ],
        compiler_params=pltpu.CompilerParams(vmem_limit_bytes=60 << 20),
        name="pack",
    )(target, coordinates, slot)

def unpack_kernel(known_ref, values_ref, place_ref, out_ref, held_ref, *, ranks, unroll):
    blocks, rows = place_ref.shape
    cells = values_ref.shape[0]
    pieces = rows // LANES
    lane = lax.broadcasted_iota(jnp.int32, (4, LANES), 1)
    down = lax.broadcasted_iota(jnp.int32, (rows, rows), 0).astype(jnp.int16)
    for i in range(cells):
        held_ref[i] = values_ref[i]
    held_ref[cells] = values_ref[0]

    def emit(k, row, whole):
        block = [jnp.zeros((4, LANES), jnp.float32)] * pieces
        for d in range(ranks):
            word = known_ref[k, ranks + d]
            cell = lax.shift_right_logical(word, 24)
            wide = jnp.full((4, LANES), word, jnp.int32)
            offset, low = wide & ((1 << 24) - 1), wide & ((1 << 14) - 1)
            for m in range(pieces if whole else 1):
                at = [jnp.minimum(cell + m + i, cells) if m else cell + i for i in (0, 1)]
                moved = pltpu.roll(jnp.where(reach(lane, 7) >= low, held_ref[at[0]], held_ref[at[1]]), word, 1)
                for i in range(m, pieces):
                    block[i] = jnp.where(reach(lane, 14, i - m) >= offset, moved, block[i])
        block = jnp.concatenate(block, axis=1)
        block = jnp.concatenate([block, jnp.zeros_like(block)], axis=0)
        at = pl.ds(pl.multiple_of(k * rows, LANES), rows)
        hot = ones_where(jnp.broadcast_to(row, (rows, rows)).astype(jnp.int16) == down)
        out_ref[:, at] = join_rows(jnp.dot(split_rows(block), hot, preferred_element_type=jnp.float32))[0:4]

    def main(g, _):
        for u in range(unroll):
            k = g * unroll + u
            emit(k, place_ref[pl.ds(k, 1), :], False)
        return 0
    for_blocks(blocks, unroll, main)

    def repair(k, _):
        @pl.when(known_ref[k, 3 * ranks] > LANES)
        def _():
            emit(k, place_ref[pl.ds(k, 1), :], True)
        return 0

    @pl.when(known_ref[0, 3 * ranks + 1] > LANES)
    def _():
        lax.fori_loop(0, blocks, repair, 0)

def unpack(words, values, place):
    blocks, rows = place.shape
    ranks, tiles = values.shape[:2]
    vm = pl.BlockSpec(memory_space=pltpu.VMEM)
    return pl.pallas_call(
        functools.partial(unpack_kernel, ranks=ranks, unroll=span_of(blocks, ranks)),
        in_specs=[pl.BlockSpec(memory_space=pltpu.SMEM), vm, vm],
        out_specs=vm,
        out_shape=jax.ShapeDtypeStruct((4, blocks * rows), jnp.float32),
        scratch_shapes=[pltpu.VMEM((ranks * tiles + 1, 4, LANES), jnp.float32)],
        compiler_params=pltpu.CompilerParams(vmem_limit_bytes=8 << 20),
        name="unpack",
    )(words, values.reshape(ranks * tiles, 4, LANES), place)

def local(fields, coordinates, element_rank, element_slot):
    ranks = lax.axis_size(("gx", "gy", "gz"))
    probes = element_slot.shape[0]
    capacity = 5 * probes // (4 * ranks)
    tiles = -(-capacity // LANES)
    rows = math.gcd(probes, 512)
    target = element_rank.reshape(probes // rows, 1, rows)
    slot = element_slot.reshape(probes // rows, 1, rows)
    send, place, words = pack(target, coordinates, slot, ranks, tiles)
    arrived = lax.all_to_all(send, ("gx", "gy", "gz"), split_axis=0, concat_axis=0, tiled=True)
    values = evaluate(arrived.reshape(ranks * tiles, 4, LANES), fields).reshape(ranks, tiles, 4, LANES)
    returned = lax.all_to_all(values, ("gx", "gy", "gz"), split_axis=0, concat_axis=0, tiled=True)
    return unpack(words, returned, place)


def solution(mesh):
    placed = (
        P(("gx", "gy", "gz"), None),
        P(None, ("gx", "gy", "gz")),
        P(("gx", "gy", "gz"), None),
        P(("gx", "gy", "gz")),
    )
    return jax.shard_map(
        local, mesh=mesh, in_specs=placed, out_specs=P(None, ("gx", "gy", "gz")), check_vma=False
    )
```
